32 devices in a mesh: gx: 4 (over x, core), gy: 4 (over z), gz: 2 (over y).
Axes of the slice: x: 2, y: 2, z: 4, core: 2. Of those that a mesh axis runs over, the one named last changes fastest.
Arguments:
- orbitals: float32 [16, 32, 32, 512], P(None, 'gx', 'gy', 'gz'), may hold values from -10 to 10
- potential: float32 [32, 32, 512], P('gx', 'gy', 'gz'), may hold values from 0 to 12
Outputs:
- updated: float32 [16, 32, 32, 512], P(None, 'gx', 'gy', 'gz')
- trial_energies: float32 [16], replicated
The draws below stay inside these ranges and needn't reach their ends.
All inputs are finite; a program needn't handle non-finite values.
Results may differ from the reference program's by a relative error of at most 0.000022.
Values sent between devices are 32-bit elements; how exact they have to be, the bound alone decides.
A program may use at most 64 MiB of HBM per device.

```python
import jax
import jax.numpy as jnp
from jax import lax

BANDS = 16
COARSE_SWEEPS = 4
NX = 32
NY = 32
NZ = 512


def draw_orbitals(key, part):
    position = jnp.arange(NX, dtype=jnp.float32) / NX
    noise = jnp.clip(jax.random.normal(jax.random.fold_in(key, 11), (BANDS, NX, NY, NZ), jnp.float32), -4.0, 4.0)
    envelope = jnp.exp(jnp.log(2.5) * position)
    return (noise * envelope[None, :, None, None]).astype(jnp.float32)


def draw_potential(key, part):
    position = jnp.arange(NX, dtype=jnp.float32) / NX
    rough = jax.random.uniform(jax.random.fold_in(key, 23), (NX, NY, NZ), jnp.float32, 0.0, 3.0)
    ramp = 6.0 * position
    return (rough + ramp[:, None, None]).astype(jnp.float32)


def setup_inputs(seed: int = 0) -> dict:
    key_list = jax.random.split(jax.random.key(seed), 3)
    orbitals = draw_orbitals(jax.random.fold_in(key_list[2], 71), 0)
    potential = draw_potential(jax.random.fold_in(key_list[2], 71), 0)
    return dict(orbitals=orbitals, potential=potential)


CENTRE_COEF = -2.5
NEAR_COEF = 4.0 / 3.0
FAR_COEF = -1.0 / 12.0
WEIGHT = 0.8
FINE_DIAG = 4.0
COARSE_DIAG = 1.75
EPSILON = 1e-6


def hamiltonian(values, potential):
    summed = (3.0 * CENTRE_COEF) * values
    for dimension in (0, 1, 2):
        summed = summed + NEAR_COEF * (jnp.roll(values, 1, dimension) + jnp.roll(values, -1, dimension))
        summed = summed + FAR_COEF * (jnp.roll(values, 2, dimension) + jnp.roll(values, -2, dimension))
    return -0.5 * summed + potential * values


def neighbours(values):
    beside_all = jnp.zeros_like(values)
    for dimension in (0, 1, 2):
        beside_all = beside_all + jnp.roll(values, 1, dimension) + jnp.roll(values, -1, dimension)
    return beside_all


def precondition(residual):
    smoothed = WEIGHT * residual / FINE_DIAG
    remainder = residual - (FINE_DIAG * smoothed - 0.5 * neighbours(smoothed))
    size_x, size_y, size_z = remainder.shape
    coarse_res = remainder.reshape(size_x // 2, 2, size_y // 2, 2, size_z // 2, 2).mean(axis=(1, 3, 5))
    approx = WEIGHT * coarse_res / COARSE_DIAG
    for sweep_index in range(COARSE_SWEEPS - 1):
        approx = approx + WEIGHT * (coarse_res - (COARSE_DIAG * approx - 0.125 * neighbours(approx))) / COARSE_DIAG
    lifted = jnp.repeat(jnp.repeat(jnp.repeat(approx, 2, 0), 2, 1), 2, 2)
    second = smoothed + lifted
    return second + WEIGHT * (residual - (FINE_DIAG * second - 0.5 * neighbours(second))) / FINE_DIAG


def one_band(wave, potential):
    applied = hamiltonian(wave, potential)
    energy = jnp.sum(wave * applied) / (jnp.sum(wave * wave) + EPSILON)
    residual = applied - energy * wave
    corrected = precondition(residual)
    applied_corr = hamiltonian(corrected, potential)
    response = applied_corr - energy * corrected
    lambda_step = -jnp.sum(residual * response) / (jnp.sum(response * response) + EPSILON)
    trial_wave = wave + lambda_step * corrected
    trial_applied = applied + lambda_step * applied_corr
    trial_energy = jnp.sum(trial_wave * trial_applied) / (jnp.sum(trial_wave * trial_wave) + EPSILON)
    residual_change = (trial_applied - trial_energy * trial_wave) - residual
    mixing_coef = -jnp.sum(residual * residual_change) / (jnp.sum(residual_change * residual_change) + EPSILON)
    mixed_res = residual + mixing_coef * residual_change
    updated = wave + (mixing_coef * lambda_step) * corrected + lambda_step * precondition(mixed_res)
    return updated, trial_energy


def reference(orbitals, potential):
    updated, trial_energies = lax.map(lambda wave: one_band(wave, potential), orbitals)
    return updated, trial_energies
```

```python
import functools

import jax
import jax.numpy as jnp
from jax import lax
from jax.experimental import pallas as pl
from jax.experimental.pallas import tpu as pltpu
from jax.sharding import PartitionSpec as P

COARSE_SWEEPS = 4
WEIGHT = 0.8
COARSE_DIAG = 1.75
EPSILON = 1e-06
LANES = 128
ROWS = 8
GROUPS = 2
AXES = ("gx", "gy", "gz")
MESH = pl.DeviceIdType.MESH
NDOTS = 8


def kernel(sizes, orb_hbm, pot, out, energies, *scratch):
    (
        orb, app, res, cor, rsp, rem, coarse,
        fys, fyr, fzs, fzr, hy, cxs, cxr, cys, cyr, czs, czr, hcy,
        acc, scal, red, load_sem, send_sem, recv_sem, rsend, rrecv,
    ) = scratch
    nx, ny, nz = sizes
    bands, xs = orb_hbm.shape[0], orb_hbm.shape[1]
    tiles = orb_hbm.shape[3] // LANES
    xc = xs // 2
    per = bands // GROUPS
    me = [lax.axis_index(a) for a in AXES]
    right = [lax.rem(m + 1, n) for m, n in zip(me, sizes)]
    left = [lax.rem(m + n - 1, n) for m, n in zip(me, sizes)]

    loads = [
        pltpu.make_async_copy(
            orb_hbm.at[:, :, :, pl.ds(t * LANES, LANES)],
            orb.at[:, pl.ds(2, xs), t],
            load_sem.at[t],
        )
        for t in range(tiles)
    ]
    for c in loads:
        c.start()
    barrier = pltpu.get_barrier_semaphore()
    for k, a in enumerate(AXES):
        for d in range(1, sizes[k]):
            pl.semaphore_signal(
                barrier, inc=1, device_id={a: lax.rem(me[k] + d, sizes[k])}, device_id_type=MESH
            )
    pl.semaphore_wait(barrier, sum(sizes) - 3)
    for c in loads:
        c.wait()

    row = lax.broadcasted_iota(jnp.int32, (ROWS, LANES), 0)
    lane = lax.broadcasted_iota(jnp.int32, (ROWS, LANES), 1)
    even_lane = lane % 2 == 0
    even_row = row % 2 == 0
    low_half = lane < LANES // 2
    first_of_four = lane % 4 < 2

    def roll(v, k, axis):
        return pltpu.roll(v, k % v.shape[axis], axis)

    def flat(ref):
        n = 1
        for s in ref.shape[:-1]:
            n *= s
        return ref.reshape(n, LANES)

    def loop(lo, hi, f):
        def step(i, carry):
            f(i)
            return carry

        lax.fori_loop(lo, hi, step, 0)

    def remote(src, dst, slot, k, axis, target):
        return pltpu.make_async_remote_copy(
            src_ref=src,
            dst_ref=dst,
            send_sem=send_sem.at[slot, k],
            recv_sem=recv_sem.at[slot, k],
            device_id={axis: target},
            device_id_type=MESH,
        )

    def z_copies(src, dst_l, dst_r, slot):
        copies = [remote(src, dst_l, slot, 4, "gz", right[2])]
        if nz > 2:
            copies.append(remote(src, dst_r, slot, 5, "gz", left[2]))
        return copies

    def fine_send(field, which, depth, g):
        lo = g * per
        view = flat(field)
        span = field.shape[1]
        ys, yr = fys[which], fyr[which]
        zs, zr = fzs[which], fzr[which]

        def pack(b):
            for t in range(tiles):
                for j in range(depth):
                    base = ((b * span + 2) * tiles + t) * ROWS
                    ys[0, b, j, t] = view[pl.ds(base + ROWS - depth + j, xs, stride=tiles * ROWS), :]
                    ys[1, b, j, t] = view[pl.ds(base + j, xs, stride=tiles * ROWS), :]
            packed = jnp.zeros((ROWS, LANES), jnp.float32)
            for x in range(xs):
                w = jnp.where(low_half, field[b, 2 + x, 0], field[b, 2 + x, tiles - 1])
                packed = jnp.where(lane // 4 == x, roll(w, 2 + 4 * x, 1), packed)
            zs[b] = packed

        loop(lo, lo + per, pack)
        slot = which * GROUPS + g
        part = pl.ds(lo, per)
        copies = [
            remote(field.at[part, pl.ds(2 + xs - depth, depth)], field.at[part, pl.ds(2 - depth, depth)], slot, 0, "gx", right[0]),
            remote(field.at[part, pl.ds(2, depth)], field.at[part, pl.ds(2 + xs, depth)], slot, 1, "gx", left[0]),
            remote(ys.at[0, part], yr.at[0, part], slot, 2, "gy", right[1]),
            remote(ys.at[1, part], yr.at[1, part], slot, 3, "gy", left[1]),
        ] + z_copies(zs.at[part], zr.at[0, part], zr.at[1, part], slot)
        for c in copies:
            c.start()
        return copies

    def wait(copies):
        for c in copies:
            c.wait()

    def z_packed(zr, b):
        if nz > 2:
            return jnp.where(first_of_four, zr[0, b], zr[1, b])
        return zr[0, b]

    def unpack_y(yr, b, depth):
        view = flat(hy)
        for t in range(tiles):
            for j in range(depth):
                base = (b * xs * tiles + t) * ROWS
                view[pl.ds(base + ROWS - depth + j, xs, stride=tiles * ROWS), :] = yr(0, j, t)
                view[pl.ds(base + j, xs, stride=tiles * ROWS), :] = yr(1, j, t)

    def shifted_y(v, h, k):
        up = roll(jnp.where(row >= ROWS - k, h, v), k, 0)
        down = roll(jnp.where(row < k, h, v), -k, 0)
        return up + down

    def shifted_z(vs, hz, k):
        before = [hz] + vs[:-1]
        after = vs[1:] + [hz]
        return [
            roll(jnp.where(lane >= LANES - k, p, v), k, 1) + roll(jnp.where(lane < k, n, v), -k, 1)
            for p, v, n in zip(before, vs, after)
        ]

    def hamiltonian(field, which, b, use):
        unpack_y(lambda s, j, t: fyr[which][s, b, j, t], b, 2)
        zp = z_packed(fzr[which], b)
        for x in range(xs):
            hz = roll(zp, -(4 * x + 2), 1)
            vs = [field[b, 2 + x, t] for t in range(tiles)]
            z1, z2 = shifted_z(vs, hz, 1), shifted_z(vs, hz, 2)
            outs = []
            for t in range(tiles):
                h = hy[b, x, t]
                near = field[b, 1 + x, t] + field[b, 3 + x, t] + shifted_y(vs[t], h, 1) + z1[t]
                far = field[b, x, t] + field[b, 4 + x, t] + shifted_y(vs[t], h, 2) + z2[t]
                potential = pot[x, :, t * LANES : (t + 1) * LANES]
                outs.append((potential + 3.75) * vs[t] - (2.0 / 3.0) * near + (1.0 / 24.0) * far)
            use(x, vs, outs)

    def rowsum(vs):
        return jnp.sum(functools.reduce(jnp.add, vs), axis=0, keepdims=True)

    def reduce_all(index, ndots):
        wide = lax.broadcasted_iota(jnp.int32, (bands, LANES), 1)
        total = jnp.zeros((bands, LANES), jnp.float32)
        for q in range(ndots):
            total = jnp.where(wide == q, jnp.sum(acc[q], axis=1, keepdims=True), total)
        for stage, k in enumerate((2, 1, 0)):
            n = sizes[k]
            buf = red.at[index * 3 + stage]
            buf[me[k]] = total
            copies = []
            for d in range(1, n):
                copies.append(
                    pltpu.make_async_remote_copy(
                        src_ref=buf.at[me[k]],
                        dst_ref=buf.at[me[k]],
                        send_sem=rsend.at[index * 3 + stage, d],
                        recv_sem=rrecv.at[index * 3 + stage, d],
                        device_id={AXES[k]: lax.rem(me[k] + d, n)},
                        device_id_type=MESH,
                    )
                )
            for c in copies:
                c.start()
            for c in copies:
                c.wait()
            total = buf[0]
            for i in range(1, n):
                total = total + buf[i]
        return [total[:, q : q + 1] for q in range(ndots)]

    def put(k, column):
        scal[k] = jnp.broadcast_to(column, (bands, LANES))

    def get(k, b):
        return scal[k, pl.ds(b, 1), :]

    def restrict(b, ry, rz):
        unpack_y(ry, b, 1)
        for X in range(xc):
            pair = [None] * tiles
            for x in (2 * X, 2 * X + 1):
                hz = roll(rz, -(4 * x + 2), 1)
                vs = [res[b, 2 + x, t] for t in range(tiles)]
                z1 = shifted_z(vs, hz, 1)
                for t in range(tiles):
                    s = res[b, 1 + x, t] + res[b, 3 + x, t] + shifted_y(vs[t], hy[b, x, t], 1) + z1[t]
                    m = (1.0 - WEIGHT) * vs[t] + (0.5 * WEIGHT / 4.0) * s
                    rem[b, x, t] = m
                    pair[t] = m if pair[t] is None else pair[t] + m
            for t in range(tiles):
                s = pair[t]
                s = s + jnp.where(even_row, roll(s, -1, 0), roll(s, 1, 0))
                s = s + jnp.where(even_lane, roll(s, -1, 1), roll(s, 1, 1))
                coarse[0, b, 1 + X, t] = s * (0.125 * WEIGHT / COARSE_DIAG)

    def coarse_send(which, level, g):
        cf = coarse.at[level]
        view = flat(coarse)
        lo = g * per // 4

        def pack(i):
            b = 4 * i
            for t in range(tiles):
                for side, X in ((0, xc), (1, 1)):
                    lanes = [
                        jnp.where(even_lane, cf[b + k, X, t], cf[b + k + 1, X, t]) for k in (0, 2)
                    ]
                    cxs[which, side, i, t] = jnp.where(even_row, lanes[0], lanes[1])
                for side, j in ((0, ROWS - 1), (1, 0)):
                    vs = [
                        view[pl.ds((((level * bands + b + k) * (xc + 2) + 1) * tiles + t) * ROWS + j, xc, stride=tiles * ROWS), :]
                        for k in range(4)
                    ]
                    ev = even_lane[:xc]
                    cys[which, side, i, t, 0:xc] = jnp.where(ev, vs[0], vs[1])
                    cys[which, side, i, t, xc : 2 * xc] = jnp.where(ev, vs[2], vs[3])

        loop(lo, lo + per // 4, pack)

        def pack_z(i):
            packed = jnp.zeros((ROWS, LANES), jnp.float32)
            for k in range(8):
                for X in range(xc):
                    off = 4 * (k * xc + X)
                    w = jnp.where(low_half, cf[8 * i + k, 1 + X, 0], cf[8 * i + k, 1 + X, tiles - 1])
                    packed = jnp.where(lane // 4 == off // 4, roll(w, 2 + off, 1), packed)
            czs[which, i] = packed

        loop(g * per // 8, (g + 1) * per // 8, pack_z)
        slot = (4 + which) * GROUPS + g
        part = pl.ds(lo, per // 4)
        zpart = pl.ds(g * per // 8, per // 8)
        copies = [
            remote(cxs.at[which, 0, part], cxr.at[which, 0, part], slot, 0, "gx", right[0]),
            remote(cxs.at[which, 1, part], cxr.at[which, 1, part], slot, 1, "gx", left[0]),
            remote(cys.at[which, 0, part], cyr.at[which, 0, part], slot, 2, "gy", right[1]),
            remote(cys.at[which, 1, part], cyr.at[which, 1, part], slot, 3, "gy", left[1]),
        ] + z_copies(czs.at[which, zpart], czr.at[which, 0, zpart], czr.at[which, 1, zpart], slot)
        for c in copies:
            c.start()
        return copies

    def spread_lanes(p):
        return (
            jnp.where(even_lane, p, roll(p, 1, 1)),
            jnp.where(even_lane, roll(p, -1, 1), p),
        )

    def coarse_unpack(which, level, g):
        cf = coarse.at[level]
        view = flat(hcy)
        lo = g * per // 4

        def unpack(i):
            b = 4 * i
            for t in range(tiles):
                for side, X in ((0, 0), (1, xc + 1)):
                    p = cxr[which, side, i, t]
                    top = jnp.where(even_row, p, roll(p, 1, 0))
                    low = jnp.where(even_row, roll(p, -1, 0), p)
                    for k, v in enumerate(spread_lanes(top) + spread_lanes(low)):
                        cf[b + k, X, t] = v
                for side, j in ((0, ROWS - 2), (1, 0)):
                    first, second = spread_lanes(cyr[which, side, i, t])
                    for k, v in enumerate((first[:xc], second[:xc], first[xc:], second[xc:])):
                        base = ((b + k) * xc * tiles + t) * ROWS + j
                        for dup in range(2):
                            view[pl.ds(base + dup, xc, stride=tiles * ROWS), :] = v

        loop(lo, lo + per // 4, unpack)

    def coarse_loop(which, g, f):
        def bundle(i):
            zp = czr[which, 0, i]
            if nz > 2:
                zp = jnp.where(first_of_four, zp, czr[which, 1, i])
            for k in range(8):
                f(8 * i + k, lambda X, k=k: roll(zp, -(4 * (k * xc + X) + 2), 1))

        loop(g * per // 8, (g + 1) * per // 8, bundle)

    def sweep(which, level, g):
        coarse_unpack(which, level, g)

        def one(b, hz):
            for X in range(xc):
                vs = [coarse[level, b, 1 + X, t] for t in range(tiles)]
                z = shifted_z(vs, hz(X), 2)
                for t in range(tiles):
                    s = coarse[level, b, X, t] + coarse[level, b, 2 + X, t] + shifted_y(vs[t], hcy[b, X, t], 2) + z[t]
                    rhs = coarse[0, b, 1 + X, t]
                    coarse[level + 1, b, 1 + X, t] = (
                        (1.0 - WEIGHT) * vs[t] + (0.125 * WEIGHT / COARSE_DIAG) * s + rhs
                    )

        coarse_loop(which, g, one)

    def prolong(which, level, g, use):
        coarse_unpack(which, level, g)

        def one(b, hz):
            for X in range(xc):
                vs = [coarse[level, b, 1 + X, t] for t in range(tiles)]
                z = shifted_z(vs, hz(X), 1)
                for t in range(tiles):
                    s = shifted_y(vs[t], hcy[b, X, t], 1) + z[t] + vs[t]
                    for x, other in ((2 * X, X), (2 * X + 1, 2 + X)):
                        total = s + coarse[level, b, other, t]
                        kr = (1.0 - WEIGHT) * (res[b, 2 + x, t] + vs[t] + rem[b, x, t]) + (
                            0.5 * WEIGHT / 4.0
                        ) * total
                        use(b, x, t, kr)

        coarse_loop(which, g, one)

    groups = range(GROUPS)

    def precondition(base, prepare, use):
        flight = []
        for g in groups:
            loop(g * per, (g + 1) * per, prepare)
            flight.append(coarse_send(base, 0, g))
        for s in range(COARSE_SWEEPS - 1):
            for g in groups:
                wait(flight[g])
                sweep(base + s, s, g)
                flight[g] = coarse_send(base + s + 1, s + 1, g)
        for g in groups:
            wait(flight[g])
            prolong(base + COARSE_SWEEPS - 1, COARSE_SWEEPS - 1, g, use)
            yield g

    flight = [fine_send(orb, 0, 2, g) for g in groups]
    second = []
    for g in groups:
        wait(flight[g])

        def apply_one(b):
            norm, energy = [], []

            def use(x, vs, outs):
                for t in range(tiles):
                    app[b, 2 + x, t] = outs[t]
                    norm.append(vs[t] * vs[t])
                    energy.append(vs[t] * outs[t])

            hamiltonian(orb, 0, b, use)
            acc[0, pl.ds(b, 1), :] = rowsum(norm)
            acc[1, pl.ds(b, 1), :] = rowsum(energy)

        loop(g * per, (g + 1) * per, apply_one)
        second.append(fine_send(app, 1, 1, g))
    norm_orbitals, first_energy = reduce_all(0, 2)
    energy = first_energy / (norm_orbitals + EPSILON)
    put(0, energy)
    for c in second:
        wait(c)

    def prepare_first(b):
        e = get(0, b)
        for x in range(1, xs + 3):
            for t in range(tiles):
                res[b, x, t] = app[b, x, t] - e * orb[b, x, t]

        def ry(s, j, t):
            return fyr[1][s, b, 0, t] - e * fyr[0][s, b, 1 - s, t]

        restrict(b, ry, z_packed(fzr[1], b) - e * z_packed(fzr[0], b))

    def use_first(b, x, t, kr):
        cor[b, 2 + x, t] = kr

    flight = []
    for g in precondition(0, prepare_first, use_first):
        flight.append(fine_send(cor, 2, 2, g))
    second = []
    for g in groups:
        wait(flight[g])

        def respond_one(b):
            e = get(0, b)
            dots = [[] for _ in range(NDOTS)]

            def use(x, vs, outs):
                for t in range(tiles):
                    c, o, r = vs[t], orb[b, 2 + x, t], res[b, 2 + x, t]
                    p = outs[t] - e * c
                    rsp[b, 2 + x, t] = p
                    for q, (u, v) in enumerate(((r, p), (p, p), (o, c), (c, c), (p, o), (p, c), (r, o), (r, c))):
                        w = u * v
                        dots[q] = [w] if not dots[q] else [dots[q][0] + w]

            hamiltonian(cor, 2, b, use)
            for q in range(NDOTS):
                acc[q, pl.ds(b, 1), :] = rowsum(dots[q])

        loop(g * per, (g + 1) * per, respond_one)
        second.append(fine_send(rsp, 3, 1, g))
    rp, pp, oc, cc, po, pc, ro, rc = reduce_all(1, NDOTS)
    lam = -rp / (pp + EPSILON)
    trial_norm = norm_orbitals + 2.0 * lam * oc + lam * lam * cc
    trial_sum = (
        first_energy + lam * ((po + energy * oc) + (rc + energy * oc)) + lam * lam * (pc + energy * cc)
    )
    trial = trial_sum / (trial_norm + EPSILON)
    energies[...] = jnp.broadcast_to(trial, (bands, LANES))
    change = trial - energy
    projected = lam * rp - change * (ro + lam * rc)
    cross = po + lam * pc
    change_norm = lam * lam * pp - 2.0 * lam * change * cross + change * change * trial_norm
    mix = -projected / (change_norm + EPSILON)
    put(1, lam)
    put(2, mix * lam)
    put(3, mix * change)
    put(4, mix * change * lam)
    for c in second:
        wait(c)

    def prepare_second(b):
        e, ml, mc, mcl = get(0, b), get(2, b), get(3, b), get(4, b)

        def mixed(r, p, o, c):
            return r + ml * p - mc * o - mcl * c

        for x in range(1, xs + 3):
            for t in range(tiles):
                res[b, x, t] = mixed(res[b, x, t], rsp[b, x, t], orb[b, x, t], cor[b, x, t])

        def ry(s, j, t):
            o = fyr[0][s, b, 1 - s, t]
            r = fyr[1][s, b, 0, t] - e * o
            return mixed(r, fyr[3][s, b, 0, t], o, fyr[2][s, b, 1 - s, t])

        oz = z_packed(fzr[0], b)
        rz = z_packed(fzr[1], b) - e * oz
        restrict(b, ry, mixed(rz, z_packed(fzr[3], b), oz, z_packed(fzr[2], b)))

    def use_second(b, x, t, kr):
        out[b, x, :, t * LANES : (t + 1) * LANES] = (
            orb[b, 2 + x, t] + get(2, b) * cor[b, 2 + x, t] + get(1, b) * kr
        )

    for g in precondition(COARSE_SWEEPS, prepare_second, use_second):
        pass


def solution(mesh):
    sizes = tuple(mesh.shape[a] for a in AXES)

    def body(orbitals, potential):
        bands, xs, ys, zs = orbitals.shape
        tiles = zs // LANES
        tile = (ROWS, LANES)
        vmem = lambda *s: pltpu.VMEM(s + tile, jnp.float32)
        field = vmem(bands, xs + 4, tiles)
        exchanges = 4 + 2 * COARSE_SWEEPS
        faces = (2 * COARSE_SWEEPS, 2, bands // 4, tiles)
        peers = max(sizes)

        def call(*refs):
            refs = list(refs)
            head, rest = refs[:4], refs[4:]
            fields, rest = rest[:7], rest[7:]
            fys, rest = rest[:4], rest[4:]
            fyr, rest = rest[:4], rest[4:]
            fzs, rest = rest[:4], rest[4:]
            fzr, rest = rest[:4], rest[4:]
            kernel(sizes, *head, *fields, fys, fyr, fzs, fzr, *rest)

        depths = (2, 1, 2, 1)
        updated, trial = pl.pallas_call(
            call,
            out_shape=(
                jax.ShapeDtypeStruct(orbitals.shape, jnp.float32),
                jax.ShapeDtypeStruct((bands, LANES), jnp.float32),
            ),
            in_specs=[
                pl.BlockSpec(memory_space=pl.ANY),
                pl.BlockSpec(memory_space=pltpu.VMEM),
            ],
            out_specs=(
                pl.BlockSpec(memory_space=pltpu.VMEM),
                pl.BlockSpec(memory_space=pltpu.VMEM),
            ),
            scratch_shapes=[field] * 5
            + [vmem(bands, xs, tiles), vmem(COARSE_SWEEPS, bands, xs // 2 + 2, tiles)]
            + [vmem(2, bands, d, tiles) for d in depths]
            + [vmem(2, bands, d, tiles) for d in depths]
            + [vmem(bands) for d in depths]
            + [vmem(2, bands) for d in depths]
            + [
                vmem(bands, xs, tiles),
                vmem(*faces),
                vmem(*faces),
                vmem(*faces),
                vmem(*faces),
                vmem(2 * COARSE_SWEEPS, bands // 8),
                vmem(2 * COARSE_SWEEPS, 2, bands // 8),
                vmem(bands, xs // 2, tiles),
                pltpu.VMEM((NDOTS, bands, LANES), jnp.float32),
                pltpu.VMEM((5, bands, LANES), jnp.float32),
                pltpu.VMEM((6, peers, bands, LANES), jnp.float32),
                pltpu.SemaphoreType.DMA((tiles,)),
                pltpu.SemaphoreType.DMA((exchanges * GROUPS, 6)),
                pltpu.SemaphoreType.DMA((exchanges * GROUPS, 6)),
                pltpu.SemaphoreType.DMA((6, peers)),
                pltpu.SemaphoreType.DMA((6, peers)),
            ],
            compiler_params=pltpu.CompilerParams(
                collective_id=0, has_side_effects=True, vmem_limit_bytes=48 * 1024 * 1024
            ),
        )(orbitals, potential)
        return updated, trial[:, 0]

    return jax.shard_map(
        body,
        mesh=mesh,
        in_specs=(P(None, "gx", "gy", "gz"), P("gx", "gy", "gz")),
        out_specs=(P(None, "gx", "gy", "gz"), P()),
        check_vma=False,
    )
```
